32 devices in a mesh: expert: 2 (over x), tensor: 16 (over z, y, core).
Axes of the slice: x: 2, y: 2, z: 4, core: 2. Of those that a mesh axis runs over, the one named last changes fastest.
Arguments:
- tokens: bfloat16 [96, 6144], P('expert', 'tensor'), may hold values from -6 to 6
- expert_ids: int32 [96, 2], P('expert'), may hold values from 0 to 1, as said below
- route_weight: int32 [96, 2], P('expert'), may hold values from 1 to 4095
- gate_weight: bfloat16 [2, 6144, 8192], P('expert', None, 'tensor'), may hold values from -0.078125 to 0.078125
- up_weight: bfloat16 [2, 6144, 8192], P('expert', None, 'tensor'), may hold values from -0.078125 to 0.078125
- down_weight: bfloat16 [2, 8192, 6144], P('expert', 'tensor'), may hold values from -0.0625 to 0.0625
Outputs:
- mixed: bfloat16 [96, 6144], P('expert', 'tensor')
- expert_load: float32 [2, 2], replicated
The draws below stay inside these ranges and needn't reach their ends.
Inputs may be any that keep to these rules, and one draw needn't show every extreme that they name: `expert_ids`: each row names two different experts. The hot expert is the one named in the first column of the first row of every aligned block of 48 rows (the tokens of one expert group), the same in all blocks. In each block exactly 48 rows name the hot expert, in either column; every other expert is named by 7 or 48 rows of each block, and by exactly 48 rows in some.
All inputs are finite; a program needn't handle non-finite values.
Results may differ from the reference program's by a relative error of at most 0.005.
Values may be sent and summed in bfloat16 or wider, within the bound.
No kernel may reach another device: no remote copies, remote signals or barrier semaphores. Data moves between devices by JAX's collectives and lax.ppermute only.
A program may use at most 64 MiB of HBM per device.

```python
import jax
import jax.numpy as jnp
from jax import lax

D = 6144
FF = 8192
TOK_DEV = 48
EXPERTS = 2
TOKENS = 96
HOT_ROWS = 48
CAP = 48


def draw_expert_ids(key, part):
    hot_id = jax.random.randint(jax.random.fold_in(key, 101), (1,), 0, EXPERTS).astype(jnp.int32)[0]
    block_count = TOKENS // TOK_DEV
    cold_count = EXPERTS - 1
    scores = jax.random.randint(jax.random.fold_in(key, 202), (block_count, TOK_DEV), 0, 1048576).astype(jnp.int32)
    scores = scores * TOK_DEV + jnp.arange(TOK_DEV, dtype=jnp.int32)[None, :]
    scores = jnp.where(jnp.arange(TOK_DEV, dtype=jnp.int32)[None, :] == 0, jnp.int32(-1), scores)
    order = jnp.argsort(scores, axis=1, stable=True).astype(jnp.int32)
    rank = jnp.argsort(order, axis=1, stable=True).astype(jnp.int32)
    rotation = jax.random.randint(jax.random.fold_in(key, 303), (block_count, 1), 0, cold_count).astype(jnp.int32)
    first_slot = jnp.where(rank < HOT_ROWS, rank, HOT_ROWS + 2 * (rank - HOT_ROWS))
    second_slot = jnp.where(rank < HOT_ROWS, rank, first_slot + 1)

    def cold_label(slot_number):
        shifted = (slot_number + rotation) % cold_count
        return shifted + (shifted >= hot_id).astype(jnp.int32)
    first = jnp.where(rank < HOT_ROWS, hot_id, cold_label(first_slot))
    second = cold_label(second_slot)
    flips = jax.random.randint(jax.random.fold_in(key, 404), (block_count, TOK_DEV), 0, 2).astype(jnp.int32)
    flips = jnp.where(jnp.arange(TOK_DEV, dtype=jnp.int32)[None, :] == 0, jnp.int32(0), flips)
    left = jnp.where(flips == 1, second, first)
    right = jnp.where(flips == 1, first, second)
    return jnp.stack([left, right], axis=2).reshape(TOKENS, 2).astype(jnp.int32)


def place_ends(array, key, low, top_value):
    spot = [jax.random.randint(jax.random.fold_in(key, axis), (), 0, length) for axis, length in enumerate(array.shape)]
    longest = array.shape.index(max(array.shape))
    neighbour = spot[:longest] + [(spot[longest] + 1) % array.shape[longest]] + spot[longest + 1:]
    return array.at[tuple(spot)].set(low).at[tuple(neighbour)].set(top_value)


def levels(key, shape, split, smallest, high):
    loudness = 1.0
    for position, parts in split:
        steps = jax.random.uniform(jax.random.fold_in(jax.random.fold_in(key, 6), position), (parts,), jnp.float32, smallest / len(split), high / len(split))
        loudness = loudness * jnp.repeat(jnp.exp(steps), shape[position] // parts).reshape((-1,) + (1,) * (len(shape) - 1 - position))
    return loudness


def centred(own_key, shape, deviation, reach, pieces=(), held_as=jnp.bfloat16):
    values = jax.random.normal(own_key, shape, jnp.float32) * deviation
    if len(pieces) > 0:
        values = levels(own_key, shape, pieces, -0.22, 0.18) * values
    return jnp.clip(values, min=-reach, max=reach).astype(held_as)


def setup_inputs(seed: int = 0) -> dict:
    streams_of = jax.random.split(jax.random.key(seed), 7)
    return {
        "tokens": centred(streams_of[0], (TOKENS, D), 1.0, 6.0, ((0, 2), (1, 16))),
        "expert_ids": draw_expert_ids(jax.random.fold_in(streams_of[6], 71), 0),
        "route_weight": place_ends(jax.random.randint(streams_of[2], (TOKENS, 2), 1, 4096), jax.random.fold_in(streams_of[2], 1), 1, 4095).astype(jnp.int32),
        "gate_weight": centred(streams_of[3], (EXPERTS, D, FF), D ** -0.5, 0.078125, ((0, 2), (2, 16))),
        "up_weight": centred(streams_of[4], (EXPERTS, D, FF), D ** -0.5, 0.078125, ((0, 2), (2, 16))),
        "down_weight": centred(streams_of[5], (EXPERTS, FF, D), FF ** -0.5, 0.0625, ((0, 2), (1, 16))),
    }


def expert_ffn(row_block, w_gate, w_up, w_down):
    gate_value = jnp.dot(row_block, w_gate, preferred_element_type=jnp.float32)
    up_value = jnp.dot(row_block, w_up, preferred_element_type=jnp.float32)
    hidden = (jax.nn.silu(gate_value) * up_value).astype(jnp.bfloat16)
    return jnp.dot(hidden, w_down, preferred_element_type=jnp.float32)


def reference(tokens, expert_ids, route_weight, gate_weight, up_weight, down_weight):
    weights = route_weight.astype(jnp.float32)
    route_share = weights / jnp.sum(weights, axis=1, keepdims=True)
    labels = jnp.arange(EXPERTS, dtype=jnp.int32)
    chosen = expert_ids[:, :, None] == labels[None, None, :]
    mixing = jnp.sum(jnp.where(chosen, route_share[:, :, None], jnp.float32(0.0)), axis=1)
    hot_id = expert_ids[0, 0]

    def add_rows(running, row_mask, most_rows, expert):
        row_index = jnp.nonzero(row_mask, size=most_rows, fill_value=0)[0].astype(jnp.int32)
        counted = jnp.sum(row_mask.astype(jnp.int32))
        is_valid = jnp.arange(most_rows, dtype=jnp.int32) < counted
        expert_out = expert_ffn(tokens[row_index], gate_weight[expert], up_weight[expert], down_weight[expert])
        row_scale = jnp.where(is_valid, mixing[row_index, expert], jnp.float32(0.0))
        return running.at[row_index].add(row_scale[:, None] * expert_out)

    running = jnp.zeros((TOKENS, D), jnp.float32)
    hot_mask = jnp.any(expert_ids == hot_id, axis=1)
    running = add_rows(running, hot_mask, EXPERTS * HOT_ROWS, hot_id)

    def cold_step(carry, expert):
        cold_mask = jnp.any(expert_ids == expert, axis=1) & (expert != hot_id)
        return add_rows(carry, cold_mask, EXPERTS * CAP, expert), None

    running, unused = lax.scan(cold_step, running, labels)
    counts = jnp.sum(chosen.astype(jnp.float32), axis=(0, 1))
    expert_load = jnp.stack([counts, jnp.sum(mixing, axis=0)]) / TOK_DEV
    return running.astype(jnp.bfloat16), expert_load
```

```python
import functools

import jax
import jax.numpy as jnp
from jax import lax
from jax.experimental import pallas as pl
from jax.experimental.pallas import tpu as pltpu
from jax.sharding import PartitionSpec as P

AXES = ("expert", "tensor")
VMEM = pl.BlockSpec(memory_space=pltpu.VMEM)
ANY = pl.BlockSpec(memory_space=pl.ANY)


def swap(value, expert_bit, tensor_mask):
    width = lax.axis_size("tensor")
    mask = expert_bit * width + tensor_mask
    pairs = [(i, i ^ mask) for i in range(2 * width)]
    return lax.ppermute(value, AXES, pairs)


def cost(flops, moved, exps=0):
    return pl.CostEstimate(flops=flops, bytes_accessed=moved, transcendentals=exps)


def gather_kernel(own, *rest):
    parts, out = (own, *rest[:-1]), rest[-1]
    for z, part in enumerate(parts):
        out[z] = part[...]


def hidden_kernel(pieces_z, *refs):
    buffers, (gate_hbm, up_hbm, out, rows, gate_w, up_w, sems) = refs[:8], refs[8:]
    tokens, width = buffers[0].shape[1:]
    here = lax.axis_index("tensor")
    pair = 2 * width
    blocks = 2 * pieces_z
    copies = []
    for block in range(blocks):
        span = pl.ds(block * pair, pair)
        for which, (hbm, held) in enumerate(((gate_hbm, gate_w), (up_hbm, up_w))):
            copy = pltpu.make_async_copy(hbm.at[0, span], held.at[span], sems.at[which, block])
            copy.start()
            copies.append(copy)
    for index, buffer in enumerate(buffers):
        group, y, core = index // 4, index // 2 % 2, index % 2
        for z in range(pieces_z):
            place = here ^ (4 * z + 2 * y + core)
            start = pl.multiple_of(place * width, 128)
            rows[pl.ds(group * tokens, tokens), pl.ds(start, width)] = buffer[z]
    gate = up = None
    for block in range(blocks):
        left = rows[:, block * pair : (block + 1) * pair]
        span = pl.ds(block * pair, pair)
        copies[2 * block].wait()
        term = jnp.dot(left, gate_w[span], preferred_element_type=jnp.float32)
        gate = term if gate is None else gate + term
        copies[2 * block + 1].wait()
        term = jnp.dot(left, up_w[span], preferred_element_type=jnp.float32)
        up = term if up is None else up + term
    out[...] = (gate / (1.0 + jnp.exp(-gate)) * up).astype(out.dtype)


def down_kernel(pieces_z, flip, hidden, down_hbm, send, keep, weights, sems):
    tokens, width = keep.shape[2:]
    here = lax.axis_index("tensor")
    core = here & 1
    pair = 2 * width
    copies = []
    for z in range(pieces_z):
        place = (here ^ (4 * z + 2 * flip)) >> 1
        span = pl.ds(pl.multiple_of(place * pair, 128), pair)
        copy = pltpu.make_async_copy(down_hbm.at[0, :, span], weights.at[z], sems.at[z])
        copy.start()
        copies.append(copy)
    left = hidden[...]
    for z in range(pieces_z):
        copies[z].wait()
        product = jnp.dot(left, weights[z], preferred_element_type=jnp.float32)
        low, high = product[:, :width], product[:, width:]
        mine = jnp.where(core == 0, low, high)
        other = jnp.where(core == 0, high, low)
        for group in range(2):
            part = slice(group * tokens, (group + 1) * tokens)
            keep[group, z] = mine[part]
            send[group, z] = other[part].astype(send.dtype)


def add_send_kernel(keep, arrived, near, far):
    near[...] = (keep[0] + arrived[0].astype(jnp.float32)).astype(near.dtype)
    far[...] = (keep[1] + arrived[1].astype(jnp.float32)).astype(far.dtype)


def add_keep_kernel(keep, arrived, near, far):
    near[...] = keep[0] + arrived[0].astype(jnp.float32)
    far[...] = (keep[1] + arrived[1].astype(jnp.float32)).astype(far.dtype)


def mix_kernel(ids, raw, own, from_y, from_x, from_xy, keep, *sends):
    expert = lax.axis_index("expert")
    weights = raw[...].astype(jnp.float32)
    share = weights / jnp.sum(weights, axis=1, keepdims=True)
    mine = jnp.sum(jnp.where(ids[...] == expert, share, 0.0), axis=1, keepdims=True)
    theirs = jnp.sum(jnp.where(ids[...] == 1 - expert, share, 0.0), axis=1, keepdims=True)
    for z in range(own.shape[0]):
        near = own[z] + from_y[z].astype(jnp.float32)
        far = from_x[z].astype(jnp.float32) + from_xy[z].astype(jnp.float32)
        total = mine * near + theirs * far
        if z == 0:
            keep[...] = total
        else:
            sends[z - 1][...] = total.astype(sends[z - 1].dtype)


def final_kernel(keep, *refs):
    total = keep[...]
    for part in refs[:-1]:
        total = total + part[...].astype(jnp.float32)
    refs[-1][...] = total.astype(refs[-1].dtype)


def call(kernel, outs, inputs, specs=None, scratch=(), estimate=None, limit=None):
    return pl.pallas_call(
        kernel,
        out_shape=outs,
        in_specs=specs or [VMEM] * len(inputs),
        out_specs=jax.tree.map(lambda _: VMEM, outs),
        scratch_shapes=list(scratch),
        cost_estimate=estimate,
        compiler_params=pltpu.CompilerParams(vmem_limit_bytes=limit),
    )(*inputs)


def dense(tokens, expert_ids, route_weight, gate_weight, up_weight, down_weight):
    rows, width = tokens.shape
    model, units = gate_weight.shape[1:]
    pieces_z = lax.axis_size("tensor") // 4
    bf16, f32 = jnp.bfloat16, jnp.float32
    shape = jax.ShapeDtypeStruct
    piece = shape((pieces_z, rows, width), bf16)
    piece32 = shape((pieces_z, rows, width), f32)

    labels = jnp.arange(2, dtype=jnp.int32)
    _, _, stats = route_stats(expert_ids, route_weight, labels)
    other_stats = swap(stats, 1, 0)

    along_z = [swap(tokens, 0, 4 * z) for z in range(1, pieces_z)]
    near = call(gather_kernel, piece, (tokens, *along_z))
    far_x = swap(near, 1, 0)
    near_y = swap(near, 0, 2)
    far_xy = swap(near, 1, 2)
    buffers = (near, near_y, far_x, far_xy)
    both = [half for buffer in buffers for half in (buffer, swap(buffer, 0, 1))]
    moved = 2 * model * units * 2
    hidden = call(
        functools.partial(hidden_kernel, pieces_z),
        shape((2 * rows, units), bf16),
        (*both, gate_weight, up_weight),
        specs=[VMEM] * 8 + [ANY] * 2,
        scratch=[
            pltpu.VMEM((2 * rows, model), bf16),
            pltpu.VMEM((model, units), bf16),
            pltpu.VMEM((model, units), bf16),
            pltpu.SemaphoreType.DMA((2, 2 * pieces_z)),
        ],
        estimate=cost(8 * rows * model * units, moved, 2 * rows * units),
        limit=40 * 2**20,
    )

    def down(flip):
        return call(
            functools.partial(down_kernel, pieces_z, flip),
            (shape((2, *piece.shape), bf16), shape((2, *piece.shape), f32)),
            (hidden, down_weight),
            specs=[VMEM, ANY],
            scratch=[
                pltpu.VMEM((pieces_z, units, 2 * width), bf16),
                pltpu.SemaphoreType.DMA((pieces_z,)),
            ],
            estimate=cost(2 * rows * model * units, model * units),
            limit=24 * 2**20,
        )

    send_far, keep_far = down(1)
    send_near, keep_near = down(0)
    got_far = swap(send_far, 0, 1)
    got_near = swap(send_near, 0, 1)
    to_y, to_xy = call(add_send_kernel, (piece, piece), (keep_far, got_far))
    own, to_x = call(add_keep_kernel, (piece32, piece), (keep_near, got_near))
    from_y = swap(to_y, 0, 2)
    from_xy = swap(to_xy, 1, 2)
    from_x = swap(to_x, 1, 0)
    small = shape((rows, width), bf16)
    keep, *sends = call(
        mix_kernel,
        (shape((rows, width), f32), *[small] * (pieces_z - 1)),
        (expert_ids, route_weight, own, from_y, from_x, from_xy),
    )
    arrived = [swap(part, 0, 4 * z) for z, part in enumerate(sends, 1)]
    mixed = call(final_kernel, small, (keep, *arrived))
    expert_load = (stats + other_stats) / rows
    return (mixed, expert_load)


def swiglu(gate_value, up_value):
    return (jax.nn.silu(gate_value) * up_value).astype(jnp.bfloat16)


def matmul(left, right):
    return jnp.dot(left, right, preferred_element_type=jnp.float32)


def route_stats(id_block, raw_block, labels):
    weights = raw_block.astype(jnp.float32)
    route_share = weights / jnp.sum(weights, axis=1, keepdims=True)
    flat_chosen = (
        (id_block[:, :, None] == labels[None, None, :])
        .astype(jnp.int32)
        .reshape(-1, labels.shape[0])
    )
    chosen_float = flat_chosen.astype(jnp.float32)
    stats = jnp.stack(
        [jnp.sum(chosen_float, axis=0), jnp.sum(route_share.reshape(-1, 1) * chosen_float, axis=0)]
    )
    return (route_share, flat_chosen, stats)


def hot_inputs(hot_local, hot_id, labels):
    is_target = (labels == hot_id)[:, None, None]
    send_rows = jnp.where(is_target, hot_local[None], jnp.zeros_like(hot_local)[None])
    arrived = lax.all_to_all(send_rows, "expert", split_axis=0, concat_axis=0, tiled=True)
    return arrived.reshape(-1, hot_local.shape[1])


def general(tokens, expert_ids, route_weight, gate_weight, up_weight, down_weight):
    tok_rows = expert_ids.shape[0]
    experts = lax.axis_size("expert") * gate_weight.shape[0]
    hot_rows = tok_rows - tok_rows // 8 * min(experts - 2, 1)
    capacity = (2 * tok_rows - hot_rows + experts - 2) // (experts - 1)
    hot_id = expert_ids[0, 0]
    own_gate = gate_weight[0]
    own_up = up_weight[0]
    own_down = down_weight[0]
    hot_gate_w, hot_up_w, hot_down_w = (own_gate, own_up, own_down)
    labels = jnp.arange(experts, dtype=jnp.int32)
    route_share, flat_chosen, local_stats = route_stats(expert_ids, route_weight, labels)
    cold_chosen = flat_chosen * (labels != hot_id).astype(jnp.int32)[None, :]
    slot_index = jnp.sum((jnp.cumsum(cold_chosen, axis=0) - 1) * cold_chosen, axis=1)
    is_live = jnp.sum(cold_chosen, axis=1)
    target = jnp.sum(cold_chosen * labels[None, :], axis=1) * capacity + slot_index
    buffer_rows = jnp.arange(experts * capacity, dtype=jnp.int32)
    cold_pick = ((target[None, :] == buffer_rows[:, None]) & (is_live[None, :] == 1)).astype(
        jnp.bfloat16
    )
    cold_pick = jnp.sum(cold_pick.reshape(experts * capacity, tok_rows, 2), axis=2)
    hot_match = (expert_ids == hot_id).astype(jnp.int32)
    hot_flag = jnp.sum(hot_match, axis=1)
    hot_rank = jnp.cumsum(hot_flag) - 1
    hot_slots = jnp.arange(hot_rows, dtype=jnp.int32)
    hot_pick = ((hot_rank[None, :] == hot_slots[:, None]) & (hot_flag[None, :] == 1)).astype(
        jnp.bfloat16
    )
    feature_width = tokens.shape[1]
    cold_send = (
        matmul(cold_pick, tokens).astype(jnp.bfloat16).reshape(experts, capacity, feature_width)
    )
    cold_recv = lax.all_to_all(
        cold_send, "expert", split_axis=0, concat_axis=0, tiled=True
    ).reshape(experts * capacity, feature_width)
    hot_input = hot_inputs(matmul(hot_pick, tokens).astype(jnp.bfloat16), hot_id, labels)
    cold_piece = lax.all_gather(cold_recv, "tensor", axis=1, tiled=True)
    hot_piece = lax.all_gather(hot_input, "tensor", axis=1, tiled=True)
    cold_gate = matmul(cold_piece, own_gate)
    cold_up = matmul(cold_piece, own_up)
    hot_gate = matmul(hot_piece, hot_gate_w)
    hot_up = matmul(hot_piece, hot_up_w)
    cold_part = matmul(swiglu(cold_gate, cold_up), own_down)
    hot_part = matmul(swiglu(hot_gate, hot_up), hot_down_w)
    model_width = cold_part.shape[1]
    came_back = lax.all_to_all(
        hot_part.reshape(experts, hot_rows, model_width),
        "expert",
        split_axis=0,
        concat_axis=0,
        tiled=True,
    )
    hot_part = lax.dynamic_index_in_dim(came_back, hot_id, 0, keepdims=False)
    returned = lax.all_to_all(
        cold_part.reshape(experts, capacity, model_width),
        "expert",
        split_axis=0,
        concat_axis=0,
        tiled=True,
    ).reshape(experts * capacity, model_width)
    assign_weight = route_share.reshape(2 * tok_rows) * is_live.astype(jnp.float32)
    cold_out = jnp.sum(
        (returned[target] * assign_weight[:, None]).reshape(tok_rows, 2, model_width), axis=1
    )
    hot_weight = jnp.sum(route_share * hot_match.astype(jnp.float32), axis=1)
    hot_out = hot_part[jnp.clip(hot_rank, 0, hot_rows - 1)] * hot_weight[:, None]
    mixed = lax.psum_scatter(cold_out + hot_out, "tensor", scatter_dimension=1, tiled=True).astype(
        jnp.bfloat16
    )
    expert_load = lax.psum(local_stats, "expert") / tok_rows
    return (mixed, expert_load)


def local(tokens, expert_ids, route_weight, gate_weight, up_weight, down_weight):
    experts = lax.axis_size("expert") * gate_weight.shape[0]
    width = lax.axis_size("tensor")
    plain = experts == lax.axis_size("expert") == 2 and width >= 8 and width & (width - 1) == 0
    layer = dense if plain else general
    return layer(tokens, expert_ids, route_weight, gate_weight, up_weight, down_weight)


def solution(mesh):
    placed = (
        P("expert", "tensor"),
        P("expert", None),
        P("expert", None),
        P("expert", None, "tensor"),
        P("expert", None, "tensor"),
        P("expert", "tensor", None),
    )
    return jax.shard_map(
        local, mesh=mesh, in_specs=placed, out_specs=(P("expert", "tensor"), P()), check_vma=False
    )
```

```python
import functools

import jax
import jax.numpy as jnp
from jax import lax
from jax.experimental import pallas as pl
from jax.experimental.pallas import tpu as pltpu
from jax.sharding import PartitionSpec as P

AXES = ("expert", "tensor")
VMEM = pl.BlockSpec(memory_space=pltpu.VMEM)
ANY = pl.BlockSpec(memory_space=pl.ANY)
LIMIT = 8 * 2**20


def swap(value, expert_bit, tensor_mask):
    width = lax.axis_size("tensor")
    mask = expert_bit * width + tensor_mask
    pairs = [(i, i ^ mask) for i in range(2 * width)]
    return lax.ppermute(value, AXES, pairs)


def cost(flops, moved, exps=0):
    return pl.CostEstimate(flops=flops, bytes_accessed=moved, transcendentals=exps)


def fetch_parts(source, held, sems):
    parts = sems.shape[-1]
    step = source.shape[1] // parts
    spans = [pl.ds(part * step, step) for part in range(parts)]
    return [
        pltpu.make_async_copy(source.at[0, span], held.at[span], sems.at[part])
        for part, span in enumerate(spans)
    ]


def enter_kernel(gate_hbm, up_hbm, tokens_hbm, gate, up, tokens, sems, token_sem):
    copies = [
        pltpu.make_async_copy(tokens_hbm, tokens, token_sem),
        *fetch_parts(gate_hbm, gate, sems.at[0]),
        *fetch_parts(up_hbm, up, sems.at[1]),
    ]
    for copy in copies:
        copy.start()
    for copy in copies:
        copy.wait()


def route_kernel(ids, raw, mixing, stats):
    expert = lax.axis_index("expert")
    weights = raw[...].astype(jnp.float32)
    share = weights / jnp.sum(weights, axis=0, keepdims=True)
    count = share.shape[1]
    shape = (count, count)
    diagonal = lax.broadcasted_iota(jnp.int32, shape, 0) == lax.broadcasted_iota(jnp.int32, shape, 1)
    for place, label in enumerate((expert, 1 - expert)):
        row = jnp.sum(jnp.where(ids[...] == label, share, 0.0), axis=0, keepdims=True)
        mixing[:, place : place + 1] = jnp.sum(jnp.where(diagonal, row, 0.0), axis=1, keepdims=True)
    for label in range(2):
        named = ids[...] == label
        for place, term in enumerate((jnp.where(named, 1.0, 0.0), jnp.where(named, share, 0.0))):
            total = jnp.sum(jnp.sum(term, axis=1, keepdims=True), axis=0, keepdims=True)
            stats[place : place + 1, label : label + 1] = total


def load_kernel(rows, stats, other_stats, load):
    load[...] = (stats[...] + other_stats[...]) / rows


def gather_kernel(*refs):
    parts, out = refs[:-3], refs[-1]
    for z, part in enumerate(parts):
        out[z] = part[...]


def hidden_kernel(pieces_z, *refs):
    buffers, (gate_w, up_w, out, rows) = refs[:8], refs[8:]
    tokens, width = buffers[0].shape[1:]
    here = lax.axis_index("tensor")
    for index, buffer in enumerate(buffers):
        group, y, core = index // 4, index // 2 % 2, index % 2
        for z in range(pieces_z):
            place = here ^ (4 * z + 2 * y + core)
            start = pl.multiple_of(place * width, 128)
            rows[pl.ds(group * tokens, tokens), pl.ds(start, width)] = buffer[z]
    left = rows[...]
    gate = jnp.dot(left, gate_w[...], preferred_element_type=jnp.float32)
    up = jnp.dot(left, up_w[...], preferred_element_type=jnp.float32)
    out[...] = (gate / (1.0 + jnp.exp(-gate)) * up).astype(out.dtype)


def down_kernel(pieces_z, flip, hidden, weights, send, keep):
    tokens, width = keep.shape[2:]
    here = lax.axis_index("tensor")
    core = here & 1
    pair = 2 * width
    left = hidden[...]
    for z in range(pieces_z):
        place = (here ^ (4 * z + 2 * flip)) >> 1
        span = pl.ds(pl.multiple_of(place * pair, 128), pair)
        product = jnp.dot(left, weights[0, :, span], preferred_element_type=jnp.float32)
        low, high = product[:, :width], product[:, width:]
        mine = jnp.where(core == 0, low, high)
        other = jnp.where(core == 0, high, low)
        for group in range(2):
            part = slice(group * tokens, (group + 1) * tokens)
            keep[group, z] = mine[part]
            send[group, z] = other[part].astype(send.dtype)


def add_send_kernel(keep, arrived, near, far):
    near[...] = (keep[0] + arrived[0].astype(jnp.float32)).astype(near.dtype)
    far[...] = (keep[1] + arrived[1].astype(jnp.float32)).astype(far.dtype)


def add_keep_kernel(keep, arrived, near, far):
    near[...] = keep[0] + arrived[0].astype(jnp.float32)
    far[...] = (keep[1] + arrived[1].astype(jnp.float32)).astype(far.dtype)


def mix_kernel(mixing, own, from_y, from_x, from_xy, keep, *sends):
    mine, theirs = mixing[:, 0:1], mixing[:, 1:2]
    for z in range(own.shape[0]):
        near = own[z] + from_y[z].astype(jnp.float32)
        far = from_x[z].astype(jnp.float32) + from_xy[z].astype(jnp.float32)
        total = mine * near + theirs * far
        if z == 0:
            keep[...] = total
        else:
            sends[z - 1][...] = total.astype(sends[z - 1].dtype)


def final_kernel(keep, *refs):
    *parts, mixed = refs
    total = keep[...]
    for part in parts:
        total = total + part[...].astype(jnp.float32)
    mixed[...] = total.astype(mixed.dtype)


def call(kernel, outs, inputs, scratch=(), estimate=None, unread=0, place=VMEM, limit=LIMIT):
    return pl.pallas_call(
        kernel,
        out_shape=outs,
        in_specs=[place] * (len(inputs) - unread) + [ANY] * unread,
        out_specs=jax.tree.map(lambda _: VMEM, outs),
        scratch_shapes=list(scratch),
        cost_estimate=estimate,
        compiler_params=pltpu.CompilerParams(vmem_limit_bytes=limit),
    )(*inputs)


def dense(tokens, expert_ids, route_weight, gate_weight, up_weight, down_weight):
    rows, width = tokens.shape
    model, units = gate_weight.shape[1:]
    pieces_z = lax.axis_size("tensor") // 4
    bf16, f32 = jnp.bfloat16, jnp.float32
    shape = jax.ShapeDtypeStruct
    piece = shape((pieces_z, rows, width), bf16)
    piece32 = shape((pieces_z, rows, width), f32)

    parts = 4
    weight = shape((model, units), bf16)
    gate_w, up_w, own_tokens = call(
        enter_kernel,
        (weight, weight, shape(tokens.shape, bf16)),
        (gate_weight, up_weight, tokens),
        scratch=[pltpu.SemaphoreType.DMA((2, parts)), pltpu.SemaphoreType.DMA],
        estimate=cost(4 * rows * model * units, 4 * model * units),
        place=ANY,
        limit=40 * 2**20,
    )
    mixing, stats = call(
        route_kernel, (shape((rows, 2), f32), shape((2, 2), f32)), (expert_ids.T, route_weight.T)
    )
    other_stats = swap(stats, 1, 0)
    along_z = [swap(tokens, 0, 4 * z) for z in range(1, pieces_z)]
    near = call(gather_kernel, piece, (own_tokens, *along_z, gate_w, up_w))
    far_x = swap(near, 1, 0)
    near_y = swap(near, 0, 2)
    far_xy = swap(near, 1, 2)
    buffers = (near, near_y, far_x, far_xy)
    both = [half for buffer in buffers for half in (buffer, swap(buffer, 0, 1))]
    moved = 2 * model * units * 2
    hidden = call(
        functools.partial(hidden_kernel, pieces_z),
        shape((2 * rows, units), bf16),
        (*both, gate_w, up_w),
        scratch=[pltpu.VMEM((2 * rows, model), bf16)],
        estimate=cost(8 * rows * model * units, moved, 2 * rows * units),
    )

    def down_call(flip):
        return call(
        functools.partial(down_kernel, pieces_z, flip),
        (shape((2, *piece.shape), bf16), shape((2, *piece.shape), f32)),
        (hidden, down_weight),
        estimate=cost(2 * rows * model * units, model * units),
        )

    send_far, keep_far = down_call(1)
    send_near, keep_near = down_call(0)
    got_far = swap(send_far, 0, 1)
    got_near = swap(send_near, 0, 1)
    to_y, to_xy = call(add_send_kernel, (piece, piece), (keep_far, got_far))
    own, to_x = call(add_keep_kernel, (piece32, piece), (keep_near, got_near))
    from_y = swap(to_y, 0, 2)
    from_xy = swap(to_xy, 1, 2)
    from_x = swap(to_x, 1, 0)
    small = shape((rows, width), bf16)
    keep, *sends = call(
        mix_kernel,
        (shape((rows, width), f32), *[small] * (pieces_z - 1)),
        (mixing, own, from_y, from_x, from_xy),
    )
    arrived = [swap(part, 0, 4 * z) for z, part in enumerate(sends, 1)]
    expert_load = call(functools.partial(load_kernel, rows), shape((2, 2), f32), (stats, other_stats))
    mixed = call(final_kernel, small, (keep, *arrived))
    return (mixed, expert_load)


def swiglu(gate_value, up_value):
    return (jax.nn.silu(gate_value) * up_value).astype(jnp.bfloat16)


def matmul(left, right):
    return jnp.dot(left, right, preferred_element_type=jnp.float32)


def route_stats(id_block, raw_block, labels):
    weights = raw_block.astype(jnp.float32)
    route_share = weights / jnp.sum(weights, axis=1, keepdims=True)
    flat_chosen = (
        (id_block[:, :, None] == labels[None, None, :])
        .astype(jnp.int32)
        .reshape(-1, labels.shape[0])
    )
    chosen_float = flat_chosen.astype(jnp.float32)
    stats = jnp.stack(
        [jnp.sum(chosen_float, axis=0), jnp.sum(route_share.reshape(-1, 1) * chosen_float, axis=0)]
    )
    return (route_share, flat_chosen, stats)


def hot_inputs(hot_local, hot_id, labels):
    is_target = (labels == hot_id)[:, None, None]
    send_rows = jnp.where(is_target, hot_local[None], jnp.zeros_like(hot_local)[None])
    arrived = lax.all_to_all(send_rows, "expert", split_axis=0, concat_axis=0, tiled=True)
    return arrived.reshape(-1, hot_local.shape[1])


def general(tokens, expert_ids, route_weight, gate_weight, up_weight, down_weight):
    tok_rows = expert_ids.shape[0]
    experts = lax.axis_size("expert") * gate_weight.shape[0]
    hot_rows = tok_rows - tok_rows // 8 * min(experts - 2, 1)
    capacity = (2 * tok_rows - hot_rows + experts - 2) // (experts - 1)
    hot_id = expert_ids[0, 0]
    own_gate = gate_weight[0]
    own_up = up_weight[0]
    own_down = down_weight[0]
    hot_gate_w, hot_up_w, hot_down_w = (own_gate, own_up, own_down)
    labels = jnp.arange(experts, dtype=jnp.int32)
    route_share, flat_chosen, local_stats = route_stats(expert_ids, route_weight, labels)
    cold_chosen = flat_chosen * (labels != hot_id).astype(jnp.int32)[None, :]
    slot_index = jnp.sum((jnp.cumsum(cold_chosen, axis=0) - 1) * cold_chosen, axis=1)
    is_live = jnp.sum(cold_chosen, axis=1)
    target = jnp.sum(cold_chosen * labels[None, :], axis=1) * capacity + slot_index
    buffer_rows = jnp.arange(experts * capacity, dtype=jnp.int32)
    cold_pick = ((target[None, :] == buffer_rows[:, None]) & (is_live[None, :] == 1)).astype(
        jnp.bfloat16
    )
    cold_pick = jnp.sum(cold_pick.reshape(experts * capacity, tok_rows, 2), axis=2)
    hot_match = (expert_ids == hot_id).astype(jnp.int32)
    hot_flag = jnp.sum(hot_match, axis=1)
    hot_rank = jnp.cumsum(hot_flag) - 1
    hot_slots = jnp.arange(hot_rows, dtype=jnp.int32)
    hot_pick = ((hot_rank[None, :] == hot_slots[:, None]) & (hot_flag[None, :] == 1)).astype(
        jnp.bfloat16
    )
    feature_width = tokens.shape[1]
    cold_send = (
        matmul(cold_pick, tokens).astype(jnp.bfloat16).reshape(experts, capacity, feature_width)
    )
    cold_recv = lax.all_to_all(
        cold_send, "expert", split_axis=0, concat_axis=0, tiled=True
    ).reshape(experts * capacity, feature_width)
    hot_input = hot_inputs(matmul(hot_pick, tokens).astype(jnp.bfloat16), hot_id, labels)
    cold_piece = lax.all_gather(cold_recv, "tensor", axis=1, tiled=True)
    hot_piece = lax.all_gather(hot_input, "tensor", axis=1, tiled=True)
    cold_gate = matmul(cold_piece, own_gate)
    cold_up = matmul(cold_piece, own_up)
    hot_gate = matmul(hot_piece, hot_gate_w)
    hot_up = matmul(hot_piece, hot_up_w)
    cold_part = matmul(swiglu(cold_gate, cold_up), own_down)
    hot_part = matmul(swiglu(hot_gate, hot_up), hot_down_w)
    model_width = cold_part.shape[1]
    came_back = lax.all_to_all(
        hot_part.reshape(experts, hot_rows, model_width),
        "expert",
        split_axis=0,
        concat_axis=0,
        tiled=True,
    )
    hot_part = lax.dynamic_index_in_dim(came_back, hot_id, 0, keepdims=False)
    returned = lax.all_to_all(
        cold_part.reshape(experts, capacity, model_width),
        "expert",
        split_axis=0,
        concat_axis=0,
        tiled=True,
    ).reshape(experts * capacity, model_width)
    assign_weight = route_share.reshape(2 * tok_rows) * is_live.astype(jnp.float32)
    cold_out = jnp.sum(
        (returned[target] * assign_weight[:, None]).reshape(tok_rows, 2, model_width), axis=1
    )
    hot_weight = jnp.sum(route_share * hot_match.astype(jnp.float32), axis=1)
    hot_out = hot_part[jnp.clip(hot_rank, 0, hot_rows - 1)] * hot_weight[:, None]
    mixed = lax.psum_scatter(cold_out + hot_out, "tensor", scatter_dimension=1, tiled=True).astype(
        jnp.bfloat16
    )
    expert_load = lax.psum(local_stats, "expert") / tok_rows
    return (mixed, expert_load)


def local(tokens, expert_ids, route_weight, gate_weight, up_weight, down_weight):
    experts = lax.axis_size("expert") * gate_weight.shape[0]
    width = lax.axis_size("tensor")
    plain = experts == lax.axis_size("expert") == 2 and width >= 8 and width & (width - 1) == 0
    if plain:
        return dense(tokens, expert_ids, route_weight, gate_weight, up_weight, down_weight)
    return general(tokens, expert_ids, route_weight, gate_weight, up_weight, down_weight)


def solution(mesh):
    placed = (
        P("expert", "tensor"),
        P("expert", None),
        P("expert", None),
        P("expert", None, "tensor"),
        P("expert", None, "tensor"),
        P("expert", "tensor", None),
    )
    return jax.shard_map(
        local, mesh=mesh, in_specs=placed, out_specs=(P("expert", "tensor"), P()), check_vma=False
    )
```

```python
import functools

import jax
import jax.numpy as jnp
from jax import lax
from jax.experimental import pallas as pl
from jax.experimental.pallas import tpu as pltpu
from jax.sharding import PartitionSpec as P

AXES = ("expert", "tensor")
VMEM = pl.BlockSpec(memory_space=pltpu.VMEM)
LIMIT = 8 * 2**20
LANES, SUBLANES = 128, 16


def swap(value, expert_bit, tensor_mask):
    width = lax.axis_size("tensor")
    mask = expert_bit * width + tensor_mask
    pairs = [(i, i ^ mask) for i in range(2 * width)]
    return lax.ppermute(value, AXES, pairs)


def cost(flops, moved, exps=0):
    return pl.CostEstimate(flops=flops, bytes_accessed=moved, transcendentals=exps)


def route_kernel(ids, raw, mixing, stats):
    expert = lax.axis_index("expert")
    weights = raw[...].astype(jnp.float32)
    share = weights / jnp.sum(weights, axis=0, keepdims=True)
    count = share.shape[1]
    shape = (count, count)
    diagonal = lax.broadcasted_iota(jnp.int32, shape, 0) == lax.broadcasted_iota(jnp.int32, shape, 1)
    for place, label in enumerate((expert, 1 - expert)):
        row = jnp.sum(jnp.where(ids[...] == label, share, 0.0), axis=0, keepdims=True)
        mixing[:, place : place + 1] = jnp.sum(jnp.where(diagonal, row, 0.0), axis=1, keepdims=True)
    stats[...] = jnp.zeros_like(stats)
    for label in range(2):
        named = ids[...] == label
        for place, term in enumerate((jnp.where(named, 1.0, 0.0), jnp.where(named, share, 0.0))):
            total = jnp.sum(jnp.sum(term, axis=1, keepdims=True), axis=0, keepdims=True)
            stats[place : place + 1, label : label + 1] = total


def early_kernel(out):
    out[...] = jnp.zeros_like(out)


def gather_kernel(*refs):
    parts, out = refs[-1 - refs[-1].shape[0] : -1], refs[-1]
    for z, part in enumerate(parts):
        out[z] = part[...]


def crossed(z):
    return int(z > 0)


def project_kernel(zs, last, *refs):
    buffers, (gate_w, up_w), refs = refs[:8], refs[8:10], refs[10:]
    tokens, width = buffers[0].shape[1:]
    rows = refs[-1]
    here = lax.axis_index("tensor")
    pair = 2 * width
    blocks = [(flip, z) for flip in range(2) for z in zs]
    for index, buffer in enumerate(buffers):
        group, flip, hop = index // 4, index // 2 % 2, index % 2
        for slot, z in enumerate(zs):
            side = (here & 1) ^ hop ^ crossed(z)
            start = pl.multiple_of(blocks.index((flip, z)) * pair + side * width, 128)
            rows[pl.ds(group * tokens, tokens), pl.ds(start, width)] = buffer[slot]
    sums = [refs[0][...], refs[1][...]] if last else [None, None]
    for block, (flip, z) in enumerate(blocks):
        left = rows[:, block * pair : (block + 1) * pair]
        place = (here ^ (4 * z + 2 * flip)) >> 1
        span = pl.ds(pl.multiple_of(place * pair, 128), pair)
        for which, weights in enumerate((gate_w, up_w)):
            term = jnp.dot(left, weights[0, span], preferred_element_type=jnp.float32)
            sums[which] = term if sums[which] is None else sums[which] + term
    gate, up = sums
    if last:
        refs[2][...] = (gate / (1.0 + jnp.exp(-gate)) * up).astype(refs[2].dtype)
    else:
        refs[1][...], refs[2][...] = gate, up


def down_kernel(zs, hidden, weights, send, keep):
    tokens, width = keep.shape[3:]
    here = lax.axis_index("tensor")
    core = here & 1
    pair = 2 * width
    left = hidden[...]
    for flip in range(2):
        for slot, z in enumerate(zs):
            place = (here ^ (4 * z + 2 * flip)) >> 1
            span = pl.ds(pl.multiple_of(place * pair, 128), pair)
            product = jnp.dot(left, weights[0, :, span], preferred_element_type=jnp.float32)
            low, high = product[:, :width], product[:, width:]
            mine = jnp.where(core == 0, low, high)
            other = jnp.where(core == 0, high, low)
            for group in range(2):
                part = slice(group * tokens, (group + 1) * tokens)
                kept, sent = (other, mine) if crossed(z) else (mine, other)
                keep[flip, group, slot] = kept[part]
                send[flip, group, slot] = sent[part].astype(send.dtype)


def add_kernel(keep, arrived, *refs):
    *stats, own, to_x, to_y, to_xy = refs
    slots, rows = own.shape[:2]
    for slot in range(slots):
        for flip, group, out in ((1, 1, to_xy), (1, 0, to_y), (0, 0, own)):
            total = keep[flip, group, slot] + arrived[flip, group, slot].astype(jnp.float32)
            out[slot] = total.astype(out.dtype)
        total = keep[0, 1, slot] + arrived[0, 1, slot].astype(jnp.float32)
        to_x[pl.ds(slot * rows, rows)] = total.astype(to_x.dtype)
    for block in stats:
        rest = block[...]
        for part in range(3):
            rounded = rest.astype(to_x.dtype)
            to_x[pl.ds(slots * rows, SUBLANES), pl.ds(part * LANES, LANES)] = rounded
            rest = rest - rounded.astype(jnp.float32)


def mix_kernel(slots, mixing, own, from_x, from_y, from_xy, *refs):
    stats, outs, load = (refs[:1], refs[1:-1], refs[-1:]) if len(refs) > slots else ((), refs, ())
    rows = mixing.shape[0]
    mine, theirs = mixing[:, 0:1], mixing[:, 1:2]
    for slot, out in enumerate(outs):
        near = own[slot] + from_y[slot].astype(jnp.float32)
        far = from_x[pl.ds(slot * rows, rows)].astype(jnp.float32) + from_xy[slot].astype(jnp.float32)
        out[...] = (mine * near + theirs * far).astype(out.dtype)
    for here, both in zip(stats, load):
        parts = [
            from_x[pl.ds(slots * rows, SUBLANES), pl.ds(part * LANES, LANES)].astype(jnp.float32)
            for part in range(3)
        ]
        both[...] = (here[...] + (parts[0] + (parts[1] + parts[2]))) / rows


def final_kernel(load, keep, *refs):
    *parts, mixed, expert_load = refs
    total = keep[...]
    for part in parts:
        total = total + part[...].astype(jnp.float32)
    mixed[...] = total.astype(mixed.dtype)
    expert_load[...] = load[: expert_load.shape[0], : expert_load.shape[1]]


def call(kernel, outs, inputs, scratch=(), estimate=None):
    return pl.pallas_call(
        kernel,
        out_shape=outs,
        in_specs=[VMEM] * len(inputs),
        out_specs=jax.tree.map(lambda _: VMEM, outs),
        scratch_shapes=list(scratch),
        cost_estimate=estimate,
        compiler_params=pltpu.CompilerParams(vmem_limit_bytes=LIMIT),
    )(*inputs)


def dense(tokens, expert_ids, route_weight, gate_weight, up_weight, down_weight):
    rows, width = tokens.shape
    model, units = gate_weight.shape[1:]
    pieces_z = lax.axis_size("tensor") // 4
    bf16, f32 = jnp.bfloat16, jnp.float32
    shape = jax.ShapeDtypeStruct

    mixing, stats = call(
        route_kernel,
        (shape((rows, 2), f32), shape((SUBLANES, LANES), f32)),
        (expert_ids.T, route_weight.T),
    )
    sets = (range(2), range(2, pieces_z))
    along_z = [tokens, *(swap(tokens, 0, 4 * z + 1) for z in range(1, pieces_z))]
    early = call(early_kernel, shape((SUBLANES, LANES), f32), (), estimate=cost(120 * rows * model * units, 0))
    both = []
    for zs in sets:
        block = shape((len(zs), rows, width), bf16)
        own = call(gather_kernel, block, [early, *(along_z[z] for z in zs)])
        moves = [(1, 0), (1, 2), (0, 2)]
        far_x, far_xy, near_y = (swap(own, x, y) for x, y in moves)
        buffers = {"own": own, "y": near_y, "x": far_x, "xy": far_xy}
        both.append([half for one in buffers.values() for half in (one, swap(one, 0, 1))])

    halves = shape((2 * rows, units), f32)
    estimate = cost(8 * rows * model * units, 2 * model * units, 2 * rows * units)
    weights = (gate_weight, up_weight)
    first = call(
        functools.partial(project_kernel, sets[0], False),
        (halves, halves),
        (*both[0], *weights, down_weight),
        scratch=[pltpu.VMEM((2 * rows, len(sets[0]) * model // pieces_z), bf16)],
        estimate=estimate,
    )
    hidden = call(
        functools.partial(project_kernel, sets[1], True),
        shape((2 * rows, units), bf16),
        (*both[1], *weights, *first),
        scratch=[pltpu.VMEM((2 * rows, len(sets[1]) * model // pieces_z), bf16)],
        estimate=estimate,
    )

    small = shape((rows, width), bf16)
    small32 = shape((rows, width), f32)
    pieces, load = {}, None
    for name, zs in (("far", sets[1]), ("near", sets[0])):
        block = (len(zs), rows, width)
        extra = [stats] if name == "far" else []
        send, keep = call(
            functools.partial(down_kernel, zs),
            (shape((2, 2, *block), bf16), shape((2, 2, *block), f32)),
            (hidden, down_weight),
            estimate=cost(2 * rows * model * units, model * units),
        )
        arrived = swap(send, 0, 1)
        own, to_x, to_y, to_xy = call(
            add_kernel,
            (
                shape(block, f32),
                shape((len(zs) * rows + len(extra) * SUBLANES, width), bf16),
                *[shape(block, bf16)] * 2,
            ),
            (keep, arrived, *extra),
        )
        from_xy = swap(to_xy, 1, 2)
        from_x = swap(to_x, 1, 0)
        from_y = swap(to_y, 0, 2)
        outs = call(
            functools.partial(mix_kernel, len(zs)),
            [*[small if z else small32 for z in zs], *[shape((SUBLANES, LANES), f32)] * len(extra)],
            (mixing, own, from_x, from_y, from_xy, *extra),
        )
        pieces.update(zip(zs, outs))
        load = outs[-1] if extra else load
    arrived = [swap(pieces[z], 0, 4 * z + 1) for z in range(pieces_z - 1, 0, -1)]
    mixed, expert_load = call(final_kernel, (small, shape((2, 2), f32)), (load, pieces[0], *arrived))
    return (mixed, expert_load)


def swiglu(gate_value, up_value):
    return (jax.nn.silu(gate_value) * up_value).astype(jnp.bfloat16)


def matmul(left, right):
    return jnp.dot(left, right, preferred_element_type=jnp.float32)


def route_stats(id_block, raw_block, labels):
    weights = raw_block.astype(jnp.float32)
    route_share = weights / jnp.sum(weights, axis=1, keepdims=True)
    flat_chosen = (
        (id_block[:, :, None] == labels[None, None, :])
        .astype(jnp.int32)
        .reshape(-1, labels.shape[0])
    )
    chosen_float = flat_chosen.astype(jnp.float32)
    stats = jnp.stack(
        [jnp.sum(chosen_float, axis=0), jnp.sum(route_share.reshape(-1, 1) * chosen_float, axis=0)]
    )
    return (route_share, flat_chosen, stats)


def hot_inputs(hot_local, hot_id, labels):
    is_target = (labels == hot_id)[:, None, None]
    send_rows = jnp.where(is_target, hot_local[None], jnp.zeros_like(hot_local)[None])
    arrived = lax.all_to_all(send_rows, "expert", split_axis=0, concat_axis=0, tiled=True)
    return arrived.reshape(-1, hot_local.shape[1])


def general(tokens, expert_ids, route_weight, gate_weight, up_weight, down_weight):
    tok_rows = expert_ids.shape[0]
    experts = lax.axis_size("expert") * gate_weight.shape[0]
    hot_rows = tok_rows - tok_rows // 8 * min(experts - 2, 1)
    capacity = (2 * tok_rows - hot_rows + experts - 2) // (experts - 1)
    hot_id = expert_ids[0, 0]
    own_gate = gate_weight[0]
    own_up = up_weight[0]
    own_down = down_weight[0]
    hot_gate_w, hot_up_w, hot_down_w = (own_gate, own_up, own_down)
    labels = jnp.arange(experts, dtype=jnp.int32)
    route_share, flat_chosen, local_stats = route_stats(expert_ids, route_weight, labels)
    cold_chosen = flat_chosen * (labels != hot_id).astype(jnp.int32)[None, :]
    slot_index = jnp.sum((jnp.cumsum(cold_chosen, axis=0) - 1) * cold_chosen, axis=1)
    is_live = jnp.sum(cold_chosen, axis=1)
    target = jnp.sum(cold_chosen * labels[None, :], axis=1) * capacity + slot_index
    buffer_rows = jnp.arange(experts * capacity, dtype=jnp.int32)
    cold_pick = ((target[None, :] == buffer_rows[:, None]) & (is_live[None, :] == 1)).astype(
        jnp.bfloat16
    )
    cold_pick = jnp.sum(cold_pick.reshape(experts * capacity, tok_rows, 2), axis=2)
    hot_match = (expert_ids == hot_id).astype(jnp.int32)
    hot_flag = jnp.sum(hot_match, axis=1)
    hot_rank = jnp.cumsum(hot_flag) - 1
    hot_slots = jnp.arange(hot_rows, dtype=jnp.int32)
    hot_pick = ((hot_rank[None, :] == hot_slots[:, None]) & (hot_flag[None, :] == 1)).astype(
        jnp.bfloat16
    )
    feature_width = tokens.shape[1]
    cold_send = (
        matmul(cold_pick, tokens).astype(jnp.bfloat16).reshape(experts, capacity, feature_width)
    )
    cold_recv = lax.all_to_all(
        cold_send, "expert", split_axis=0, concat_axis=0, tiled=True
    ).reshape(experts * capacity, feature_width)
    hot_input = hot_inputs(matmul(hot_pick, tokens).astype(jnp.bfloat16), hot_id, labels)
    cold_piece = lax.all_gather(cold_recv, "tensor", axis=1, tiled=True)
    hot_piece = lax.all_gather(hot_input, "tensor", axis=1, tiled=True)
    cold_gate = matmul(cold_piece, own_gate)
    cold_up = matmul(cold_piece, own_up)
    hot_gate = matmul(hot_piece, hot_gate_w)
    hot_up = matmul(hot_piece, hot_up_w)
    cold_part = matmul(swiglu(cold_gate, cold_up), own_down)
    hot_part = matmul(swiglu(hot_gate, hot_up), hot_down_w)
    model_width = cold_part.shape[1]
    came_back = lax.all_to_all(
        hot_part.reshape(experts, hot_rows, model_width),
        "expert",
        split_axis=0,
        concat_axis=0,
        tiled=True,
    )
    hot_part = lax.dynamic_index_in_dim(came_back, hot_id, 0, keepdims=False)
    returned = lax.all_to_all(
        cold_part.reshape(experts, capacity, model_width),
        "expert",
        split_axis=0,
        concat_axis=0,
        tiled=True,
    ).reshape(experts * capacity, model_width)
    assign_weight = route_share.reshape(2 * tok_rows) * is_live.astype(jnp.float32)
    cold_out = jnp.sum(
        (returned[target] * assign_weight[:, None]).reshape(tok_rows, 2, model_width), axis=1
    )
    hot_weight = jnp.sum(route_share * hot_match.astype(jnp.float32), axis=1)
    hot_out = hot_part[jnp.clip(hot_rank, 0, hot_rows - 1)] * hot_weight[:, None]
    mixed = lax.psum_scatter(cold_out + hot_out, "tensor", scatter_dimension=1, tiled=True).astype(
        jnp.bfloat16
    )
    expert_load = lax.psum(local_stats, "expert") / tok_rows
    return (mixed, expert_load)


def local(tokens, expert_ids, route_weight, gate_weight, up_weight, down_weight):
    experts = lax.axis_size("expert") * gate_weight.shape[0]
    width = lax.axis_size("tensor")
    width_ok = tokens.shape[1] >= 3 * LANES
    plain = width_ok and experts == lax.axis_size("expert") == 2 and width >= 16 and width & (width - 1) == 0
    if plain:
        return dense(tokens, expert_ids, route_weight, gate_weight, up_weight, down_weight)
    return general(tokens, expert_ids, route_weight, gate_weight, up_weight, down_weight)


def solution(mesh):
    placed = (
        P("expert", "tensor"),
        P("expert", None),
        P("expert", None),
        P("expert", None, "tensor"),
        P("expert", None, "tensor"),
        P("expert", "tensor", None),
    )
    return jax.shard_map(
        local, mesh=mesh, in_specs=placed, out_specs=(P("expert", "tensor"), P()), check_vma=False
    )
```

```python
import functools

import jax
import jax.numpy as jnp
from jax import lax
from jax.experimental import pallas as pl
from jax.experimental.pallas import tpu as pltpu
from jax.sharding import PartitionSpec as P

AXES = ("expert", "tensor")
VMEM = pl.BlockSpec(memory_space=pltpu.VMEM)
LIMIT = 8 * 2**20
LANES, SUBLANES = 128, 16


def swap(value, expert_bit, tensor_mask):
    width = lax.axis_size("tensor")
    mask = expert_bit * width + tensor_mask
    pairs = [(i, i ^ mask) for i in range(2 * width)]
    return lax.ppermute(value, AXES, pairs)


def cost(flops, moved, exps=0):
    return pl.CostEstimate(flops=flops, bytes_accessed=moved, transcendentals=exps)


def route_kernel(ids, raw, mixing, stats):
    expert = lax.axis_index("expert")
    weights = raw[...].astype(jnp.float32)
    share = weights / jnp.sum(weights, axis=0, keepdims=True)
    count = share.shape[1]
    shape = (count, count)
    diagonal = lax.broadcasted_iota(jnp.int32, shape, 0) == lax.broadcasted_iota(jnp.int32, shape, 1)
    for place, label in enumerate((expert, 1 - expert)):
        row = jnp.sum(jnp.where(ids[...] == label, share, 0.0), axis=0, keepdims=True)
        mixing[:, place : place + 1] = jnp.sum(jnp.where(diagonal, row, 0.0), axis=1, keepdims=True)
    stats[...] = jnp.zeros_like(stats)
    for label in range(2):
        named = ids[...] == label
        for place, term in enumerate((jnp.where(named, 1.0, 0.0), jnp.where(named, share, 0.0))):
            total = jnp.sum(jnp.sum(term, axis=1, keepdims=True), axis=0, keepdims=True)
            stats[place : place + 1, label : label + 1] = total


def early_kernel(out):
    out[...] = jnp.zeros_like(out)


def gather_kernel(*refs):
    parts, out = refs[-1 - refs[-1].shape[0] : -1], refs[-1]
    for z, part in enumerate(parts):
        out[z] = part[...]


def crossed(z):
    return int(z > 0)


def project_kernel(zs, last, *refs):
    buffers, (gate_w, up_w), refs = refs[:8], refs[8:10], refs[10:]
    tokens, width = buffers[0].shape[1:]
    rows = refs[-1]
    here = lax.axis_index("tensor")
    pair = 2 * width
    blocks = [(flip, z) for flip in range(2) for z in zs]
    for index, buffer in enumerate(buffers):
        group, flip, hop = index // 4, index // 2 % 2, index % 2
        for slot, z in enumerate(zs):
            side = (here & 1) ^ hop ^ crossed(z)
            start = pl.multiple_of(blocks.index((flip, z)) * pair + side * width, 128)
            rows[pl.ds(group * tokens, tokens), pl.ds(start, width)] = buffer[slot]
    sums = [refs[0][...], refs[1][...]] if last else [None, None]
    for block, (flip, z) in enumerate(blocks):
        left = rows[:, block * pair : (block + 1) * pair]
        place = (here ^ (4 * z + 2 * flip)) >> 1
        span = pl.ds(pl.multiple_of(place * pair, 128), pair)
        for which, weights in enumerate((gate_w, up_w)):
            term = jnp.dot(left, weights[0, span], preferred_element_type=jnp.float32)
            sums[which] = term if sums[which] is None else sums[which] + term
    gate, up = sums
    if last:
        refs[2][...] = (gate / (1.0 + jnp.exp(-gate)) * up).astype(refs[2].dtype)
    else:
        refs[1][...], refs[2][...] = gate, up


def down_kernel(zs, hidden, weights, send, keep):
    tokens, width = keep.shape[3:]
    here = lax.axis_index("tensor")
    core = here & 1
    pair = 2 * width
    left = hidden[...]
    for flip in range(2):
        for slot, z in enumerate(zs):
            place = (here ^ (4 * z + 2 * flip)) >> 1
            span = pl.ds(pl.multiple_of(place * pair, 128), pair)
            product = jnp.dot(left, weights[0, :, span], preferred_element_type=jnp.float32)
            low, high = product[:, :width], product[:, width:]
            mine = jnp.where(core == 0, low, high)
            other = jnp.where(core == 0, high, low)
            for group in range(2):
                part = slice(group * tokens, (group + 1) * tokens)
                kept, sent = (other, mine) if crossed(z) else (mine, other)
                keep[flip, group, slot] = kept[part]
                send[flip, group, slot] = sent[part].astype(send.dtype)


def project_down_kernel(zs, *refs):
    inputs, down_w, (hidden, send, keep, rows) = refs[:12], refs[12], refs[13:]
    project_kernel(zs, True, *inputs, hidden, rows)
    down_kernel(zs, hidden, down_w, send, keep)


def add_kernel(keep, arrived, *refs):
    *stats, own, to_x, to_y, to_xy = refs
    slots, rows = own.shape[:2]
    for slot in range(slots):
        for flip, group, out in ((1, 1, to_xy), (1, 0, to_y), (0, 0, own)):
            total = keep[flip, group, slot] + arrived[flip, group, slot].astype(jnp.float32)
            out[slot] = total.astype(out.dtype)
        total = keep[0, 1, slot] + arrived[0, 1, slot].astype(jnp.float32)
        to_x[pl.ds(slot * rows, rows)] = total.astype(to_x.dtype)
    for block in stats:
        rest = block[...]
        for part in range(3):
            rounded = rest.astype(to_x.dtype)
            to_x[pl.ds(slots * rows, SUBLANES), pl.ds(part * LANES, LANES)] = rounded
            rest = rest - rounded.astype(jnp.float32)


def mix_kernel(slots, mixing, own, from_x, from_y, from_xy, *refs):
    stats, outs, load = (refs[:1], refs[1:-1], refs[-1:]) if len(refs) > slots else ((), refs, ())
    rows = mixing.shape[0]
    mine, theirs = mixing[:, 0:1], mixing[:, 1:2]
    for slot, out in enumerate(outs):
        near = own[slot] + from_y[slot].astype(jnp.float32)
        far = from_x[pl.ds(slot * rows, rows)].astype(jnp.float32) + from_xy[slot].astype(jnp.float32)
        out[...] = (mine * near + theirs * far).astype(out.dtype)
    for here, both in zip(stats, load):
        parts = [
            from_x[pl.ds(slots * rows, SUBLANES), pl.ds(part * LANES, LANES)].astype(jnp.float32)
            for part in range(3)
        ]
        both[...] = (here[...] + (parts[0] + (parts[1] + parts[2]))) / rows


def final_kernel(load, keep, *refs):
    *parts, mixed, expert_load = refs
    total = keep[...]
    for part in parts:
        total = total + part[...].astype(jnp.float32)
    mixed[...] = total.astype(mixed.dtype)
    expert_load[...] = load[: expert_load.shape[0], : expert_load.shape[1]]


def call(kernel, outs, inputs, scratch=(), estimate=None):
    return pl.pallas_call(
        kernel,
        out_shape=outs,
        in_specs=[VMEM] * len(inputs),
        out_specs=jax.tree.map(lambda _: VMEM, outs),
        scratch_shapes=list(scratch),
        cost_estimate=estimate,
        compiler_params=pltpu.CompilerParams(vmem_limit_bytes=LIMIT),
    )(*inputs)


def dense(tokens, expert_ids, route_weight, gate_weight, up_weight, down_weight):
    rows, width = tokens.shape
    model, units = gate_weight.shape[1:]
    pieces_z = lax.axis_size("tensor") // 4
    bf16, f32 = jnp.bfloat16, jnp.float32
    shape = jax.ShapeDtypeStruct

    mixing, stats = call(
        route_kernel,
        (shape((rows, 2), f32), shape((SUBLANES, LANES), f32)),
        (expert_ids.T, route_weight.T),
    )
    sets = (range(2), range(2, pieces_z))
    along_z = [tokens, *(swap(tokens, 0, 4 * z + 1) for z in range(1, pieces_z))]
    early = call(early_kernel, shape((SUBLANES, LANES), f32), (), estimate=cost(120 * rows * model * units, 0))
    both = []
    for zs in sets:
        block = shape((len(zs), rows, width), bf16)
        own = call(gather_kernel, block, [early, *(along_z[z] for z in zs)])
        moves = [(1, 0), (1, 2), (0, 2)]
        far_x, far_xy, near_y = (swap(own, x, y) for x, y in moves)
        buffers = {"own": own, "y": near_y, "x": far_x, "xy": far_xy}
        both.append([half for one in buffers.values() for half in (one, swap(one, 0, 1))])

    halves = shape((2 * rows, units), f32)
    estimate = cost(8 * rows * model * units, 2 * model * units, 2 * rows * units)
    weights = (gate_weight, up_weight)
    first = call(
        functools.partial(project_kernel, sets[0], False),
        (halves, halves),
        (*both[0], *weights, down_weight),
        scratch=[pltpu.VMEM((2 * rows, len(sets[0]) * model // pieces_z), bf16)],
        estimate=estimate,
    )
    far_block = (2, 2, len(sets[1]), rows, width)
    hidden, *far_parts = call(
        functools.partial(project_down_kernel, sets[1]),
        (shape((2 * rows, units), bf16), shape(far_block, bf16), shape(far_block, f32)),
        (*both[1], *weights, *first, down_weight),
        scratch=[pltpu.VMEM((2 * rows, len(sets[1]) * model // pieces_z), bf16)],
        estimate=estimate,
    )

    small = shape((rows, width), bf16)
    small32 = shape((rows, width), f32)
    pieces, load = {}, None
    for name, zs in (("far", sets[1]), ("near", sets[0])):
        block = (len(zs), rows, width)
        extra = [stats] if name == "far" else []
        if name == "far":
            send, keep = far_parts
        else:
            send, keep = call(
                functools.partial(down_kernel, zs),
                (shape((2, 2, *block), bf16), shape((2, 2, *block), f32)),
                (hidden, down_weight),
                estimate=cost(2 * rows * model * units, model * units),
            )
        arrived = swap(send, 0, 1)
        own, to_x, to_y, to_xy = call(
            add_kernel,
            (
                shape(block, f32),
                shape((len(zs) * rows + len(extra) * SUBLANES, width), bf16),
                *[shape(block, bf16)] * 2,
            ),
            (keep, arrived, *extra),
        )
        from_xy = swap(to_xy, 1, 2)
        from_x = swap(to_x, 1, 0)
        from_y = swap(to_y, 0, 2)
        outs = call(
            functools.partial(mix_kernel, len(zs)),
            [*[small if z else small32 for z in zs], *[shape((SUBLANES, LANES), f32)] * len(extra)],
            (mixing, own, from_x, from_y, from_xy, *extra),
        )
        pieces.update(zip(zs, outs))
        load = outs[-1] if extra else load
    arrived = [swap(pieces[z], 0, 4 * z + 1) for z in range(pieces_z - 1, 0, -1)]
    mixed, expert_load = call(final_kernel, (small, shape((2, 2), f32)), (load, pieces[0], *arrived))
    return (mixed, expert_load)


def swiglu(gate_value, up_value):
    return (jax.nn.silu(gate_value) * up_value).astype(jnp.bfloat16)


def matmul(left, right):
    return jnp.dot(left, right, preferred_element_type=jnp.float32)


def route_stats(id_block, raw_block, labels):
    weights = raw_block.astype(jnp.float32)
    route_share = weights / jnp.sum(weights, axis=1, keepdims=True)
    flat_chosen = (
        (id_block[:, :, None] == labels[None, None, :])
        .astype(jnp.int32)
        .reshape(-1, labels.shape[0])
    )
    chosen_float = flat_chosen.astype(jnp.float32)
    stats = jnp.stack(
        [jnp.sum(chosen_float, axis=0), jnp.sum(route_share.reshape(-1, 1) * chosen_float, axis=0)]
    )
    return (route_share, flat_chosen, stats)


def hot_inputs(hot_local, hot_id, labels):
    is_target = (labels == hot_id)[:, None, None]
    send_rows = jnp.where(is_target, hot_local[None], jnp.zeros_like(hot_local)[None])
    arrived = lax.all_to_all(send_rows, "expert", split_axis=0, concat_axis=0, tiled=True)
    return arrived.reshape(-1, hot_local.shape[1])


def general(tokens, expert_ids, route_weight, gate_weight, up_weight, down_weight):
    tok_rows = expert_ids.shape[0]
    experts = lax.axis_size("expert") * gate_weight.shape[0]
    hot_rows = tok_rows - tok_rows // 8 * min(experts - 2, 1)
    capacity = (2 * tok_rows - hot_rows + experts - 2) // (experts - 1)
    hot_id = expert_ids[0, 0]
    own_gate = gate_weight[0]
    own_up = up_weight[0]
    own_down = down_weight[0]
    hot_gate_w, hot_up_w, hot_down_w = (own_gate, own_up, own_down)
    labels = jnp.arange(experts, dtype=jnp.int32)
    route_share, flat_chosen, local_stats = route_stats(expert_ids, route_weight, labels)
    cold_chosen = flat_chosen * (labels != hot_id).astype(jnp.int32)[None, :]
    slot_index = jnp.sum((jnp.cumsum(cold_chosen, axis=0) - 1) * cold_chosen, axis=1)
    is_live = jnp.sum(cold_chosen, axis=1)
    target = jnp.sum(cold_chosen * labels[None, :], axis=1) * capacity + slot_index
    buffer_rows = jnp.arange(experts * capacity, dtype=jnp.int32)
    cold_pick = ((target[None, :] == buffer_rows[:, None]) & (is_live[None, :] == 1)).astype(
        jnp.bfloat16
    )
    cold_pick = jnp.sum(cold_pick.reshape(experts * capacity, tok_rows, 2), axis=2)
    hot_match = (expert_ids == hot_id).astype(jnp.int32)
    hot_flag = jnp.sum(hot_match, axis=1)
    hot_rank = jnp.cumsum(hot_flag) - 1
    hot_slots = jnp.arange(hot_rows, dtype=jnp.int32)
    hot_pick = ((hot_rank[None, :] == hot_slots[:, None]) & (hot_flag[None, :] == 1)).astype(
        jnp.bfloat16
    )
    feature_width = tokens.shape[1]
    cold_send = (
        matmul(cold_pick, tokens).astype(jnp.bfloat16).reshape(experts, capacity, feature_width)
    )
    cold_recv = lax.all_to_all(
        cold_send, "expert", split_axis=0, concat_axis=0, tiled=True
    ).reshape(experts * capacity, feature_width)
    hot_input = hot_inputs(matmul(hot_pick, tokens).astype(jnp.bfloat16), hot_id, labels)
    cold_piece = lax.all_gather(cold_recv, "tensor", axis=1, tiled=True)
    hot_piece = lax.all_gather(hot_input, "tensor", axis=1, tiled=True)
    cold_gate = matmul(cold_piece, own_gate)
    cold_up = matmul(cold_piece, own_up)
    hot_gate = matmul(hot_piece, hot_gate_w)
    hot_up = matmul(hot_piece, hot_up_w)
    cold_part = matmul(swiglu(cold_gate, cold_up), own_down)
    hot_part = matmul(swiglu(hot_gate, hot_up), hot_down_w)
    model_width = cold_part.shape[1]
    came_back = lax.all_to_all(
        hot_part.reshape(experts, hot_rows, model_width),
        "expert",
        split_axis=0,
        concat_axis=0,
        tiled=True,
    )
    hot_part = lax.dynamic_index_in_dim(came_back, hot_id, 0, keepdims=False)
    returned = lax.all_to_all(
        cold_part.reshape(experts, capacity, model_width),
        "expert",
        split_axis=0,
        concat_axis=0,
        tiled=True,
    ).reshape(experts * capacity, model_width)
    assign_weight = route_share.reshape(2 * tok_rows) * is_live.astype(jnp.float32)
    cold_out = jnp.sum(
        (returned[target] * assign_weight[:, None]).reshape(tok_rows, 2, model_width), axis=1
    )
    hot_weight = jnp.sum(route_share * hot_match.astype(jnp.float32), axis=1)
    hot_out = hot_part[jnp.clip(hot_rank, 0, hot_rows - 1)] * hot_weight[:, None]
    mixed = lax.psum_scatter(cold_out + hot_out, "tensor", scatter_dimension=1, tiled=True).astype(
        jnp.bfloat16
    )
    expert_load = lax.psum(local_stats, "expert") / tok_rows
    return (mixed, expert_load)


def local(tokens, expert_ids, route_weight, gate_weight, up_weight, down_weight):
    experts = lax.axis_size("expert") * gate_weight.shape[0]
    width = lax.axis_size("tensor")
    width_ok = tokens.shape[1] >= 3 * LANES
    plain = width_ok and experts == lax.axis_size("expert") == 2 and width >= 16 and width & (width - 1) == 0
    if plain:
        return dense(tokens, expert_ids, route_weight, gate_weight, up_weight, down_weight)
    return general(tokens, expert_ids, route_weight, gate_weight, up_weight, down_weight)


def solution(mesh):
    placed = (
        P("expert", "tensor"),
        P("expert", None),
        P("expert", None),
        P("expert", None, "tensor"),
        P("expert", None, "tensor"),
        P("expert", "tensor", None),
    )
    return jax.shard_map(
        local, mesh=mesh, in_specs=placed, out_specs=(P("expert", "tensor"), P()), check_vma=False
    )
```
